256 devices in a mesh: row: 8 (over x, z_lo), col: 8 (over z_hi, core), depth: 4 (over y).
Axes of the slice: x: 4, y: 4, z: 8 (z_hi: 4, z_lo: 2; z = z_hi * 2 + z_lo), core: 2. Of those that a mesh axis runs over, the one named last changes fastest.
Arguments:
- alignment_matrix: bfloat16 [128, 768, 256], P('depth', 'col'), may hold values from -6 to 6
- twin_linear_matrix: bfloat16 [256, 64], replicated, may hold values from -0.375 to 0.375
- final_matrix: bfloat16 [1024, 128], replicated, may hold values from -2 to 2
- final_offset: float32 [128], replicated, may hold values from -3 to 3
- adjoint_incoming: bfloat16 [768, 768, 128], P('row', ('col', 'depth')), may hold values from -6 to 6
Outputs:
- contact_delta: bfloat16 [768, 768, 128], P('row', ('col', 'depth'))
- alignment_adjoint: float32 [128, 768, 256], P('depth', 'col')
- grad_w_out: float32 [1024, 128], replicated
- grad_b_out: float32 [128], replicated
The draws below stay inside these ranges and needn't reach their ends.
All inputs are finite; a program needn't handle non-finite values.
Results may differ from the reference program's by a relative error of at most 0.007.
Values may be sent and summed in bfloat16 or wider, within the bound.
No kernel may reach another device: no remote copies, remote signals or barrier semaphores. Data moves between devices by JAX's collectives and lax.ppermute only.
A program may use at most 128 MiB of HBM per device.

```python
import jax
import jax.numpy as jnp
from jax import lax

ALIGN_FEATURES = 256
HIDDEN_CHANNELS = 32
CONTACT_FEATURES = 128
RES = 96
ALIGNMENT_ROWS = 128
KRONECKER_SIZE = 1024
AMINO_ACID_COUNT = 768


def block_levels(own_key, shape, shards, least, high):
    def one(dim, blocks):
        heights = jax.random.uniform(jax.random.fold_in(jax.random.fold_in(own_key, 6), dim), (blocks,), jnp.float32, least / len(shards), high / len(shards))
        return jnp.repeat(jnp.exp(heights), shape[dim] // blocks).reshape((-1,) + (1,) * (len(shape) - dim - 1))

    loudness = one(*shards[0])
    for cut in shards[1:]:
        loudness = loudness * one(*cut)
    return loudness


def scatter_about(key, extent, width, bound, split=(), kind=jnp.bfloat16):
    result = width * jax.random.normal(key, extent, jnp.float32)
    if split:
        result = result * block_levels(key, extent, split, -0.22, 0.18)
    return jnp.clip(result, -bound, bound).astype(kind)


def setup_inputs(seed: int = 0) -> dict:
    key_of = jax.random.split(jax.random.key(seed), 6)
    alignment_matrix = scatter_about(key_of[0], (ALIGNMENT_ROWS, AMINO_ACID_COUNT, ALIGN_FEATURES), 1.0, 6.0, ((0, 4), (1, 8)))
    twin_linear_matrix = scatter_about(key_of[1], (ALIGN_FEATURES, 2 * HIDDEN_CHANNELS), ALIGN_FEATURES ** -0.5, 0.375)
    final_matrix = scatter_about(key_of[2], (KRONECKER_SIZE, CONTACT_FEATURES), (KRONECKER_SIZE // ALIGNMENT_ROWS) ** -0.5, 2.0)
    final_offset = scatter_about(key_of[3], (CONTACT_FEATURES,), 0.5, 3.0, (), jnp.float32)
    adjoint_incoming = scatter_about(key_of[4], (AMINO_ACID_COUNT, AMINO_ACID_COUNT, CONTACT_FEATURES), 1.0, 6.0, ((0, 8), (1, 32)))
    return {"alignment_matrix": alignment_matrix, "twin_linear_matrix": twin_linear_matrix, "final_matrix": final_matrix, "final_offset": final_offset, "adjoint_incoming": adjoint_incoming}


epsilon = 1e-05

def standardize_channels(values):
    centre = lax.optimization_barrier(jnp.mean(values, axis=-1, keepdims=True))
    spread = lax.optimization_barrier(jnp.mean(jnp.square(values - centre), axis=-1, keepdims=True))
    return (values - centre) * lax.rsqrt(spread + epsilon)

def reference(alignment_matrix, twin_linear_matrix, final_matrix, final_offset, adjoint_incoming):
    latent_features = twin_linear_matrix.shape[1] // 2
    standardized_alignment, standardize_backprop = jax.vjp(standardize_channels, alignment_matrix.astype(jnp.float32))
    normed = standardized_alignment.astype(jnp.bfloat16)
    panels = jnp.dot(normed, twin_linear_matrix, preferred_element_type=jnp.float32).astype(jnp.bfloat16)
    left = panels[..., :latent_features].astype(jnp.float32)
    right = panels[..., latent_features:].astype(jnp.float32)
    blocks = AMINO_ACID_COUNT // RES

    def one_block(state_acc, step_index):
        matrix_accumulator, offset_accumulator, right_acc = state_acc
        offset = (step_index * RES).astype(jnp.int32)
        rows_left = lax.dynamic_slice_in_dim(left, offset, RES, 1)
        kronecker_tile = jnp.einsum('sic,sje->ijce', rows_left, right).reshape(RES, AMINO_ACID_COUNT, KRONECKER_SIZE)
        kronecker_tile = (kronecker_tile / ALIGNMENT_ROWS).astype(jnp.bfloat16)
        pair_blk = (jnp.dot(kronecker_tile, final_matrix, preferred_element_type=jnp.float32) + final_offset).astype(jnp.bfloat16)
        adjoint_tile = lax.dynamic_slice_in_dim(adjoint_incoming, offset, RES, 0).astype(jnp.float32)
        adjoint_kronecker = (jnp.einsum('gtz,vz->gtv', adjoint_tile, final_matrix.astype(jnp.float32)) / ALIGNMENT_ROWS).astype(jnp.bfloat16)
        grad_four = adjoint_kronecker.astype(jnp.float32).reshape(RES, AMINO_ACID_COUNT, latent_features, latent_features)
        left_blk = jnp.einsum('ijce,sje->sic', grad_four, right)
        right_acc = right_acc + jnp.einsum('ijce,sic->sje', grad_four, rows_left)
        matrix_accumulator = matrix_accumulator + jnp.einsum('ijf,ijo->fo', kronecker_tile.astype(jnp.float32), adjoint_tile)
        offset_accumulator = offset_accumulator + lax.optimization_barrier(jnp.sum(adjoint_tile, axis=(0, 1)))
        return ((matrix_accumulator, offset_accumulator, right_acc), (pair_blk, left_blk))
    initial_carry = (jnp.zeros((KRONECKER_SIZE, CONTACT_FEATURES), jnp.float32), jnp.zeros((CONTACT_FEATURES,), jnp.float32), jnp.zeros((ALIGNMENT_ROWS, AMINO_ACID_COUNT, latent_features), jnp.float32))
    final_state, stacked = lax.scan(one_block, initial_carry, jnp.arange(blocks, dtype=jnp.int32))
    matrix_accumulator, offset_accumulator, right_acc = final_state
    pair_blocks, leftside_tiles = stacked
    contact_delta = pair_blocks.reshape(AMINO_ACID_COUNT, AMINO_ACID_COUNT, CONTACT_FEATURES)
    adjoint_leftside = jnp.transpose(leftside_tiles, (1, 0, 2, 3)).reshape(ALIGNMENT_ROWS, AMINO_ACID_COUNT, latent_features)
    grad_panels = jnp.concatenate([adjoint_leftside, right_acc], axis=-1).astype(jnp.bfloat16)
    standardized_adjoint = jnp.dot(grad_panels, jnp.transpose(twin_linear_matrix), preferred_element_type=jnp.float32)
    alignment_adjoint = standardize_backprop(standardized_adjoint)[0]
    return (contact_delta, alignment_adjoint, matrix_accumulator / AMINO_ACID_COUNT, offset_accumulator / AMINO_ACID_COUNT)
```

```python
import jax
import jax.numpy as jnp
from jax import lax
from jax.experimental import pallas as pl
from jax.experimental.pallas import tpu as pltpu
from jax.sharding import PartitionSpec as P


epsilon = 1e-05
BF, F32 = jnp.bfloat16, jnp.float32
PLANE = ("row", "col")
TN = (((0,), (0,)), ((), ()))
NT = (((1,), (1,)), ((), ()))


def lane_mean(values):
    share = jnp.full((values.shape[-1], 128), 1.0 / values.shape[-1], BF)
    high = values.astype(BF)
    mean = jnp.dot(high, share, preferred_element_type=F32)
    if values.dtype == F32:
        low = (values - high.astype(F32)).astype(BF)
        mean = mean + jnp.dot(low, share, preferred_element_type=F32)
    return jnp.concatenate([mean, mean], axis=-1)


def standardized(rows):
    centred = rows.astype(F32) - lane_mean(rows)
    factor = lax.rsqrt(lane_mean(jnp.square(centred)) + epsilon)
    return centred * factor, factor


def panels_kernel(align_ref, weights_ref, left_ref, right_ref):
    share, amino, width = align_ref.shape
    latent = weights_ref.shape[0] // 2
    left_w, right_w = weights_ref[:latent], weights_ref[latent:]
    normed, _ = standardized(align_ref[...].reshape(share * amino, width))
    normed = normed.astype(BF)
    right = lax.dot_general(normed, right_w, NT, preferred_element_type=F32)
    right_ref[...] = right.astype(BF).reshape(right_ref.shape)
    for s in range(share):
        rows = normed[s * amino : (s + 1) * amino]
        left_ref[s] = lax.dot_general(left_w, rows, NT, preferred_element_type=F32).astype(BF)


def panels_of(align, weights):
    share, amino, width = align.shape
    latent = weights.shape[0] // 2
    whole = pl.BlockSpec((2 * latent, width), lambda g: (0, 0))
    return pl.pallas_call(
        panels_kernel,
        grid=(share // 8,),
        in_specs=[pl.BlockSpec((8, amino, width), lambda g: (g, 0, 0)), whole],
        out_specs=[
            pl.BlockSpec((8, latent, amino), lambda g: (g, 0, 0)),
            pl.BlockSpec((8, amino, latent), lambda g: (g, 0, 0)),
        ],
        out_shape=[
            jax.ShapeDtypeStruct((share, latent, amino), BF),
            jax.ShapeDtypeStruct((share, amino, latent), BF),
        ],
        name="panels",
    )(align, weights)


def align_kernel(align_ref, left_ref, right_ref, weights_ref, out_ref):
    share, amino, width = align_ref.shape
    latent = weights_ref.shape[0] // 2
    left_w, right_w = weights_ref[:latent], weights_ref[latent:]
    normed, factor = standardized(align_ref[...].reshape(share * amino, width))
    grad = jnp.concatenate([lax.dot_general(left_ref[s], left_w, TN, preferred_element_type=F32) for s in range(share)])
    right = right_ref[...].reshape(share * amino, latent)
    grad = grad + jnp.dot(right, right_w, preferred_element_type=F32)
    result = factor * (grad - lane_mean(grad) - normed * lane_mean(grad * normed))
    out_ref[...] = result.reshape(out_ref.shape)


def align_of(align, left_grad, right_grad, weights):
    share, amino, width = align.shape
    latent = weights.shape[0] // 2
    whole = pl.BlockSpec((2 * latent, width), lambda g: (0, 0))
    return pl.pallas_call(
        align_kernel,
        grid=(share // 8,),
        in_specs=[
            pl.BlockSpec((8, amino, width), lambda g: (g, 0, 0)),
            pl.BlockSpec((8, latent, amino), lambda g: (g, 0, 0)),
            pl.BlockSpec((8, amino, latent), lambda g: (g, 0, 0)),
            whole,
        ],
        out_specs=pl.BlockSpec((8, amino, width), lambda g: (g, 0, 0)),
        out_shape=jax.ShapeDtypeStruct(align.shape, F32),
        name="align",
    )(align, left_grad, right_grad, weights)


def swap_blocks(tiles):
    t0, t1, t2, t3 = tiles
    lane = lax.broadcasted_iota(jnp.int32, t0.shape, 1)
    half, quarter = (lane & 64) == 0, (lane & 32) == 0
    a0, a2 = jnp.where(half, t0, pltpu.roll(t2, 64, 1)), jnp.where(half, pltpu.roll(t0, 64, 1), t2)
    a1, a3 = jnp.where(half, t1, pltpu.roll(t3, 64, 1)), jnp.where(half, pltpu.roll(t1, 64, 1), t3)
    return (
        jnp.where(quarter, a0, pltpu.roll(a1, 32, 1)),
        jnp.where(quarter, pltpu.roll(a0, 96, 1), a1),
        jnp.where(quarter, a2, pltpu.roll(a3, 32, 1)),
        jnp.where(quarter, pltpu.roll(a2, 96, 1), a3),
    )


def grad_outer_kernel(scale, adj_ref, final_ref, right_ref, outer_ref, left_ref):
    quarter, block_i, width = adj_ref.shape
    final = final_ref[...]
    for four in range(quarter // 4):
        adj = adj_ref[four * 4 : (four + 1) * 4].reshape(4 * block_i, width)
        g = lax.dot_general(adj, final, NT, preferred_element_type=F32) * scale
        tiles = [g[j * block_i : (j + 1) * block_i] for j in range(4)]
        for c, tile in enumerate(swap_blocks(tiles)):
            outer_ref[c * block_i : (c + 1) * block_i, four * 128 : (four + 1) * 128] = tile.astype(BF)
    left_ref[...] = lax.dot_general(right_ref[...], outer_ref[...], NT, preferred_element_type=F32).astype(BF)


def grad_outer_of(adj, final, right, scale):
    _, block_i, width = adj.shape
    seqs, lanes = right.shape
    groups = final.shape[0] // 128
    return pl.pallas_call(
        lambda *refs: grad_outer_kernel(scale, *refs),
        grid=(groups,),
        in_specs=[
            pl.BlockSpec(adj.shape, lambda g: (0, 0, 0)),
            pl.BlockSpec((128, width), lambda g: (g, 0)),
            pl.BlockSpec(right.shape, lambda g: (0, 0)),
        ],
        out_specs=[
            pl.BlockSpec((4 * block_i, lanes), lambda g: (g, 0)),
            pl.BlockSpec((seqs, 4 * block_i), lambda g: (0, g)),
        ],
        out_shape=[
            jax.ShapeDtypeStruct((groups * 4 * block_i, lanes), BF),
            jax.ShapeDtypeStruct((seqs, groups * 4 * block_i), BF),
        ],
        name="grad_outer",
    )(adj, final, right)


def outer_kernel(scale, left_ref, right_ref, adj_ref, final_ref, offset_ref, pair_ref, weight_ref, outer_ref):
    step = pl.program_id(0)
    quarter, block_i, width = adj_ref.shape
    column = pl.ds(pl.multiple_of(step * 128, 128), 128)
    left = left_ref[...]
    for pair in range(quarter // 8):
        o = lax.dot_general(left, right_ref[:, pair * 256 : (pair + 1) * 256], TN, preferred_element_type=F32) * scale
        for part in range(2):
            tiles = [o[c * block_i : (c + 1) * block_i, part * 128 : (part + 1) * 128] for c in range(4)]
            for j, tile in enumerate(swap_blocks(tiles)):
                at = ((pair * 2 + part) * 4 + j) * block_i
                outer_ref[at : at + block_i, column] = tile.astype(BF)

    @pl.when(step == pl.num_programs(0) - 1)
    def _():
        weight = None
        for pair in range(quarter // 8):
            rows = slice(pair * 8 * block_i, (pair + 1) * 8 * block_i)
            outer = outer_ref[rows, :]
            adj = adj_ref[pair * 8 : (pair + 1) * 8].reshape(8 * block_i, width)
            pairs = jnp.dot(outer, final_ref[...], preferred_element_type=F32) + offset_ref[...]
            pair_ref[pair * 8 : (pair + 1) * 8] = pairs.astype(BF).reshape(8, block_i, width)
            part = lax.dot_general(adj, outer, TN, preferred_element_type=F32)
            weight = part if weight is None else weight + part
        weight_ref[...] = weight.T.astype(BF)


def outer_of(left, right, adj, final, offset, scale):
    quarter, block_i, width = adj.shape
    seqs = left.shape[0]
    whole = lambda shape: pl.BlockSpec(shape, lambda g: (0,) * len(shape))
    return pl.pallas_call(
        lambda *refs: outer_kernel(scale, *refs),
        grid=(left.shape[1] // (4 * block_i),),
        in_specs=[
            pl.BlockSpec((seqs, 4 * block_i), lambda g: (0, g)),
            whole(right.shape),
            whole(adj.shape),
            whole(final.shape),
            whole((1, width)),
        ],
        out_specs=[whole(adj.shape), whole(final.shape)],
        out_shape=[jax.ShapeDtypeStruct(adj.shape, BF), jax.ShapeDtypeStruct(final.shape, BF)],
        scratch_shapes=[pltpu.VMEM((quarter * block_i, final.shape[0]), BF)],
        name="outer",
    )(left, right, adj, final, offset.reshape(1, width))


def shifted(value, axis, by):
    n = lax.axis_size(axis)
    return lax.ppermute(value, axis, [(q, (q + by) % n) for q in range(n)])


def crossings():
    pairs = []
    for row in range(8):
        for col in range(8):
            source_row = ((col // 2 + row // 2) % 4) * 2 + col % 2
            pairs.append((source_row * 8 + row, row * 8 + col))
    return pairs


def exchange(pieces, axis):
    return lax.all_to_all(pieces, axis, split_axis=0, concat_axis=0, tiled=True)


def copies(piece, n):
    return jnp.broadcast_to(piece[None], (n, *piece.shape))


def step(alignment_matrix, twin_linear_matrix, final_matrix, final_offset, adjoint_incoming):
    share, amino, _ = alignment_matrix.shape
    latent = twin_linear_matrix.shape[1] // 2
    depth_count = lax.axis_size("depth")
    row_count = lax.axis_size("row")
    plane_count = row_count * lax.axis_size("col")
    crop_length = amino * lax.axis_size("col")
    _, quarter, width = adjoint_incoming.shape
    kron = final_matrix.shape[0]
    seq_count = share * depth_count
    there = crossings()
    back = [(b, a) for a, b in there]

    weights_t = twin_linear_matrix.T
    left_own, right_own = panels_of(alignment_matrix, weights_t)
    left_mine = lax.ppermute(left_own.reshape(share, latent * amino), PLANE, there)
    right_own = right_own.reshape(share, depth_count, quarter * latent).transpose(1, 0, 2)
    right = exchange(right_own, "depth").reshape(seq_count, quarter * latent)

    adj = jnp.transpose(adjoint_incoming, (1, 0, 2))
    adj, right, left_mine = lax.optimization_barrier((adj, right, left_mine))
    left = exchange(copies(left_mine, depth_count), "depth").reshape(seq_count, latent * amino)
    grad_outer, grad_left = grad_outer_of(adj, final_matrix, right, 1.0 / seq_count)
    grad_right = lax.dot_general(left, grad_outer, (((1,), (0,)), ((), ())), preferred_element_type=F32).astype(BF)
    grads = jnp.concatenate([grad_left, grad_right], axis=-1).reshape(depth_count, share, -1)
    grads = exchange(grads, "depth")
    pair_t, weight = outer_of(left, right, adj, final_matrix, final_offset, 1.0 / seq_count)
    contact_delta = jnp.transpose(pair_t, (1, 0, 2))

    left_sum = jnp.sum(grads[..., : latent * amino].astype(F32), axis=0).astype(BF)
    weight, left_sum = lax.optimization_barrier((weight, left_sum))
    left_part = lax.ppermute(left_sum, PLANE, back)
    piece = latent * amino // row_count
    left_pieces = left_part.reshape(share, row_count, piece).transpose(1, 0, 2)
    right_pieces = grads[..., latent * amino :].reshape(depth_count, share, row_count // depth_count, piece)
    right_pieces = right_pieces.transpose(0, 2, 1, 3).reshape(row_count, share, piece)
    pieces = jnp.concatenate([left_pieces, right_pieces], axis=-1)
    turned = lax.dynamic_slice_in_dim(jnp.concatenate([pieces, pieces]), lax.axis_index("row"), row_count, 0)
    reduced = turned[0].astype(F32)
    for k in range(1, row_count):
        reduced = reduced + shifted(turned[k], "row", k).astype(F32)
    reduced = reduced.astype(BF)
    grads = exchange(copies(reduced, row_count), "row")
    left_full = grads[..., :piece].reshape(row_count, share, latent // row_count, amino)
    left_full = left_full.transpose(1, 0, 2, 3).reshape(share, latent, amino)
    right_full = grads[..., piece:].reshape(row_count, share, amino // row_count, latent)
    right_full = right_full.transpose(1, 0, 2, 3).reshape(share, amino, latent)
    alignment_adjoint = align_of(alignment_matrix, left_full, right_full, weights_t)

    bias = jnp.sum(adjoint_incoming.astype(F32), axis=(0, 1)).astype(BF)
    rows = kron // plane_count
    bias_rows = jnp.broadcast_to(bias[None, None], (plane_count, 8, width))
    sent = jnp.concatenate([weight.reshape(plane_count, rows, width), bias_rows], axis=1)
    received = exchange(sent, PLANE)
    mine = jnp.sum(received.astype(F32), axis=0)
    total = ((mine + shifted(mine, "depth", 2)) + (shifted(mine, "depth", 1) + shifted(mine, "depth", 3))) / crop_length
    weight_gradient = exchange(copies(total[:rows].astype(BF), plane_count), PLANE)
    weight_gradient = weight_gradient.reshape(kron, width).astype(F32)
    return contact_delta, alignment_adjoint, weight_gradient, total[rows]


def solution(mesh):
    in_specs = (P("depth", "col", None), P(), P(), P(), P("row", ("col", "depth"), None))
    out_specs = (P("row", ("col", "depth"), None), P("depth", "col", None), P(), P())
    return jax.shard_map(step, mesh=mesh, in_specs=in_specs, out_specs=out_specs, check_vma=False)
```

```python
import jax
import jax.numpy as jnp
from jax import lax
from jax.experimental import pallas as pl
from jax.experimental.pallas import tpu as pltpu
from jax.sharding import PartitionSpec as P


epsilon = 1e-05
BF, F32 = jnp.bfloat16, jnp.float32
PLANE = ("row", "col")
TN = (((0,), (0,)), ((), ()))
NT = (((1,), (1,)), ((), ()))


def lane_mean(values):
    share = jnp.full((values.shape[-1], 128), 1.0 / values.shape[-1], BF)
    high = values.astype(BF)
    mean = jnp.dot(high, share, preferred_element_type=F32)
    if values.dtype == F32:
        low = (values - high.astype(F32)).astype(BF)
        mean = mean + jnp.dot(low, share, preferred_element_type=F32)
    return jnp.concatenate([mean, mean], axis=-1)


def standardized(rows):
    centred = rows.astype(F32) - lane_mean(rows)
    factor = lax.rsqrt(lane_mean(jnp.square(centred)) + epsilon)
    return centred * factor, factor


def panels_kernel(align_ref, weights_ref, left_ref, right_ref):
    share, amino, width = align_ref.shape
    latent = weights_ref.shape[0] // 2
    left_w, right_w = weights_ref[:latent], weights_ref[latent:]
    normed, _ = standardized(align_ref[...].reshape(share * amino, width))
    normed = normed.astype(BF)
    right = lax.dot_general(normed, right_w, NT, preferred_element_type=F32)
    right_ref[...] = right.astype(BF).reshape(right_ref.shape)
    for s in range(share):
        rows = normed[s * amino : (s + 1) * amino]
        left_ref[s] = lax.dot_general(left_w, rows, NT, preferred_element_type=F32).astype(BF)


def panels_of(align, weights):
    share, amino, width = align.shape
    latent = weights.shape[0] // 2
    whole = pl.BlockSpec((2 * latent, width), lambda g: (0, 0))
    return pl.pallas_call(
        panels_kernel,
        grid=(share // 8,),
        in_specs=[pl.BlockSpec((8, amino, width), lambda g: (g, 0, 0)), whole],
        out_specs=[
            pl.BlockSpec((8, latent, amino), lambda g: (g, 0, 0)),
            pl.BlockSpec((8, amino, latent), lambda g: (g, 0, 0)),
        ],
        out_shape=[
            jax.ShapeDtypeStruct((share, latent, amino), BF),
            jax.ShapeDtypeStruct((share, amino, latent), BF),
        ],
        name="panels",
    )(align, weights)


def align_kernel(align_ref, left_ref, right_ref, weights_ref, out_ref):
    share, amino, width = align_ref.shape
    latent = weights_ref.shape[0] // 2
    left_w, right_w = weights_ref[:latent], weights_ref[latent:]
    normed, factor = standardized(align_ref[...].reshape(share * amino, width))
    grad = jnp.concatenate([lax.dot_general(left_ref[s], left_w, TN, preferred_element_type=F32) for s in range(share)])
    right = right_ref[...].reshape(share * amino, latent)
    grad = grad + jnp.dot(right, right_w, preferred_element_type=F32)
    result = factor * (grad - lane_mean(grad) - normed * lane_mean(grad * normed))
    out_ref[...] = result.reshape(out_ref.shape)


def align_of(align, left_grad, right_grad, weights):
    share, amino, width = align.shape
    latent = weights.shape[0] // 2
    whole = pl.BlockSpec((2 * latent, width), lambda g: (0, 0))
    return pl.pallas_call(
        align_kernel,
        grid=(share // 8,),
        in_specs=[
            pl.BlockSpec((8, amino, width), lambda g: (g, 0, 0)),
            pl.BlockSpec((8, latent, amino), lambda g: (g, 0, 0)),
            pl.BlockSpec((8, amino, latent), lambda g: (g, 0, 0)),
            whole,
        ],
        out_specs=pl.BlockSpec((8, amino, width), lambda g: (g, 0, 0)),
        out_shape=jax.ShapeDtypeStruct(align.shape, F32),
        name="align",
    )(align, left_grad, right_grad, weights)


def swap_blocks(tiles):
    t0, t1, t2, t3 = tiles
    lane = lax.broadcasted_iota(jnp.int32, t0.shape, 1)
    half, quarter = (lane & 64) == 0, (lane & 32) == 0
    a0, a2 = jnp.where(half, t0, pltpu.roll(t2, 64, 1)), jnp.where(half, pltpu.roll(t0, 64, 1), t2)
    a1, a3 = jnp.where(half, t1, pltpu.roll(t3, 64, 1)), jnp.where(half, pltpu.roll(t1, 64, 1), t3)
    return (
        jnp.where(quarter, a0, pltpu.roll(a1, 32, 1)),
        jnp.where(quarter, pltpu.roll(a0, 96, 1), a1),
        jnp.where(quarter, a2, pltpu.roll(a3, 32, 1)),
        jnp.where(quarter, pltpu.roll(a2, 96, 1), a3),
    )


def grad_outer_kernel(scale, adj_ref, final_ref, right_ref, outer_ref, left_ref):
    quarter, block_i, width = adj_ref.shape
    final = final_ref[...]
    for four in range(quarter // 4):
        adj = adj_ref[four * 4 : (four + 1) * 4].reshape(4 * block_i, width)
        g = lax.dot_general(adj, final, NT, preferred_element_type=F32).astype(BF)
        for part in range(final.shape[0] // 128):
            tiles = [g[j * block_i : (j + 1) * block_i, part * 128 : (part + 1) * 128] for j in range(4)]
            for c, tile in enumerate(swap_blocks(tiles)):
                at = (part * 4 + c) * block_i
                outer_ref[at : at + block_i, four * 128 : (four + 1) * 128] = tile
    left = lax.dot_general(right_ref[...], outer_ref[...], NT, preferred_element_type=F32)
    left_ref[...] = (left * scale).astype(BF)


def grad_outer_of(adj, final, right, scale):
    _, block_i, width = adj.shape
    seqs, lanes = right.shape
    groups = final.shape[0] // 256
    return pl.pallas_call(
        lambda *refs: grad_outer_kernel(scale, *refs),
        grid=(groups,),
        in_specs=[
            pl.BlockSpec(adj.shape, lambda g: (0, 0, 0)),
            pl.BlockSpec((256, width), lambda g: (g, 0)),
            pl.BlockSpec(right.shape, lambda g: (0, 0)),
        ],
        out_specs=[
            pl.BlockSpec((8 * block_i, lanes), lambda g: (g, 0)),
            pl.BlockSpec((seqs, 8 * block_i), lambda g: (0, g)),
        ],
        out_shape=[
            jax.ShapeDtypeStruct((groups * 8 * block_i, lanes), BF),
            jax.ShapeDtypeStruct((seqs, groups * 8 * block_i), BF),
        ],
        name="grad_outer",
    )(adj, final, right)


def outer_kernel(scale, left_ref, right_ref, adj_ref, final_ref, offset_ref, pair_ref, weight_ref, outer_ref):
    step = pl.program_id(0)
    quarter, block_i, width = adj_ref.shape
    column = pl.ds(pl.multiple_of(step * 128, 128), 128)
    left = left_ref[...]
    for pair in range(quarter // 8):
        o = lax.dot_general(left, right_ref[:, pair * 256 : (pair + 1) * 256], TN, preferred_element_type=F32).astype(BF)
        for part in range(2):
            tiles = [o[c * block_i : (c + 1) * block_i, part * 128 : (part + 1) * 128] for c in range(4)]
            for j, tile in enumerate(swap_blocks(tiles)):
                at = ((pair * 2 + part) * 4 + j) * block_i
                outer_ref[at : at + block_i, column] = tile

    @pl.when(step == pl.num_programs(0) - 1)
    def _():
        weight = None
        for pair in range(quarter // 8):
            rows = slice(pair * 8 * block_i, (pair + 1) * 8 * block_i)
            outer = outer_ref[rows, :]
            adj = adj_ref[pair * 8 : (pair + 1) * 8].reshape(8 * block_i, width)
            pairs = jnp.dot(outer, final_ref[...], preferred_element_type=F32) * scale + offset_ref[...]
            pair_ref[pair * 8 : (pair + 1) * 8] = pairs.astype(BF).reshape(8, block_i, width)
            part = lax.dot_general(adj, outer, TN, preferred_element_type=F32)
            weight = part if weight is None else weight + part
        weight = (weight * scale).T.astype(BF)
        bias = jnp.sum(adj_ref[...].astype(F32).reshape(quarter * block_i, width), axis=0, keepdims=True)
        bias = jnp.broadcast_to(bias.astype(BF), (8, width))
        pieces, rows = weight_ref.shape[0], weight_ref.shape[1] - 8
        for p in range(pieces):
            weight_ref[p] = jnp.concatenate([weight[p * rows : (p + 1) * rows], bias])


def outer_of(left, right, adj, final, offset, scale, pieces):
    quarter, block_i, width = adj.shape
    weight = (pieces, final.shape[0] // pieces + 8, width)
    seqs = left.shape[0]
    whole = lambda shape: pl.BlockSpec(shape, lambda g: (0,) * len(shape))
    return pl.pallas_call(
        lambda *refs: outer_kernel(scale, *refs),
        grid=(left.shape[1] // (4 * block_i),),
        in_specs=[
            pl.BlockSpec((seqs, 4 * block_i), lambda g: (0, g)),
            whole(right.shape),
            whole(adj.shape),
            whole(final.shape),
            whole((1, width)),
        ],
        out_specs=[whole(adj.shape), whole(weight)],
        out_shape=[jax.ShapeDtypeStruct(adj.shape, BF), jax.ShapeDtypeStruct(weight, BF)],
        scratch_shapes=[pltpu.VMEM((quarter * block_i, final.shape[0]), BF)],
        name="outer",
    )(left, right, adj, final, offset.reshape(1, width))


def shifted(value, axis, by):
    n = lax.axis_size(axis)
    return lax.ppermute(value, axis, [(q, (q + by) % n) for q in range(n)])


def crossings():
    pairs = []
    for row in range(8):
        for col in range(8):
            source_row = ((row + 2 - col // 2 - row % 2) % 4) * 2 + col % 2
            pairs.append((source_row * 8 + row, row * 8 + col))
    return pairs


def exchange(pieces, axis):
    return lax.all_to_all(pieces, axis, split_axis=0, concat_axis=0, tiled=True)


def copies(piece, n):
    return jnp.broadcast_to(piece[None], (n, *piece.shape))


def step(alignment_matrix, twin_linear_matrix, final_matrix, final_offset, adjoint_incoming):
    share, amino, _ = alignment_matrix.shape
    latent = twin_linear_matrix.shape[1] // 2
    depth_count = lax.axis_size("depth")
    row_count = lax.axis_size("row")
    plane_count = row_count * lax.axis_size("col")
    crop_length = amino * lax.axis_size("col")
    _, quarter, width = adjoint_incoming.shape
    kron = final_matrix.shape[0]
    seq_count = share * depth_count
    depth_idx = lax.axis_index("depth")
    there = crossings()
    back = [(b, a) for a, b in there]

    weights_t = twin_linear_matrix.T
    left_own, right_own = panels_of(alignment_matrix, weights_t)
    left_mine = lax.ppermute(left_own.reshape(share, latent * amino), PLANE, there)
    right_own = right_own.reshape(share, depth_count, quarter * latent).transpose(1, 0, 2)
    right = exchange(right_own, "depth")

    def turned_back(chunks):
        chunks = chunks.reshape(depth_count, share, -1)[::-1]
        start = depth_count - 1 - depth_idx
        return lax.dynamic_slice_in_dim(jnp.concatenate([chunks, chunks]), start, depth_count, 0)

    right_turned = turned_back(right).reshape(seq_count, quarter * latent)
    right = right.reshape(seq_count, quarter * latent)

    adj = jnp.transpose(adjoint_incoming, (1, 0, 2))
    adj, left_mine = lax.optimization_barrier((adj, left_mine))
    left = jnp.concatenate([left_mine] + [shifted(left_mine, "depth", k) for k in range(1, depth_count)])
    grad_outer, grad_left = grad_outer_of(adj, final_matrix, right, 1.0 / seq_count)
    grad_right = lax.dot_general(left, grad_outer, (((1,), (0,)), ((), ())), preferred_element_type=F32)
    grad_right = (grad_right / seq_count).astype(BF)
    grad_left = grad_left.reshape(depth_count, share, latent * amino)
    grads = exchange(jnp.concatenate([grad_left, turned_back(grad_right)], axis=-1), "depth")
    pair_t, weight = outer_of(left, right_turned, adj, final_matrix, final_offset, 1.0 / seq_count, plane_count)
    contact_delta = jnp.transpose(pair_t, (1, 0, 2))

    left_sum = jnp.sum(grads[..., : latent * amino].astype(F32), axis=0).astype(BF)
    weight, left_sum = lax.optimization_barrier((weight, left_sum))
    left_part = lax.ppermute(left_sum, PLANE, back)
    piece = latent * amino // row_count
    left_pieces = left_part.reshape(share, row_count, piece).transpose(1, 0, 2)
    right_pieces = grads[..., latent * amino :].reshape(depth_count, share, row_count // depth_count, piece)
    right_pieces = right_pieces.transpose(0, 2, 1, 3).reshape(row_count, share, piece)
    pieces = jnp.concatenate([left_pieces, right_pieces], axis=-1)
    turned = lax.dynamic_slice_in_dim(jnp.concatenate([pieces, pieces]), lax.axis_index("row"), row_count, 0)
    reduced = turned[0].astype(F32)
    for k in range(1, row_count):
        reduced = reduced + shifted(turned[k], "row", k).astype(F32)
    reduced = reduced.astype(BF)
    grads = exchange(copies(reduced, row_count), "row")
    left_full = grads[..., :piece].reshape(row_count, share, latent // row_count, amino)
    left_full = left_full.transpose(1, 0, 2, 3).reshape(share, latent, amino)
    right_full = grads[..., piece:].reshape(row_count, share, amino // row_count, latent)
    right_full = right_full.transpose(1, 0, 2, 3).reshape(share, amino, latent)
    alignment_adjoint = align_of(alignment_matrix, left_full, right_full, weights_t)

    rows = kron // plane_count
    received = exchange(weight, PLANE)
    mine = jnp.sum(received.astype(F32), axis=0)
    total = ((mine + shifted(mine, "depth", 2)) + (shifted(mine, "depth", 1) + shifted(mine, "depth", 3))) / crop_length
    weight_gradient = exchange(copies(total[:rows].astype(BF), plane_count), PLANE)
    weight_gradient = weight_gradient.reshape(kron, width).astype(F32)
    return contact_delta, alignment_adjoint, weight_gradient, total[rows]


def solution(mesh):
    in_specs = (P("depth", "col", None), P(), P(), P(), P("row", ("col", "depth"), None))
    out_specs = (P("row", ("col", "depth"), None), P("depth", "col", None), P(), P())
    return jax.shard_map(step, mesh=mesh, in_specs=in_specs, out_specs=out_specs, check_vma=False)
```

```python
import jax
import jax.numpy as jnp
from jax import lax
from jax.experimental import pallas as pl
from jax.experimental.pallas import tpu as pltpu
from jax.sharding import PartitionSpec as P


epsilon = 1e-05
BF, F32 = jnp.bfloat16, jnp.float32
PLANE = ("row", "col")
TN = (((0,), (0,)), ((), ()))
NT = (((1,), (1,)), ((), ()))


def lane_mean(values):
    return jnp.mean(values.astype(F32), axis=-1, keepdims=True)


def standardized(rows):
    centred = rows.astype(F32) - lane_mean(rows)
    factor = lax.rsqrt(lane_mean(jnp.square(centred)) + epsilon)
    return centred * factor, factor


def panels_kernel(align_ref, weights_ref, left_ref, right_ref):
    share, amino, width = align_ref.shape
    latent = weights_ref.shape[0] // 2
    left_w, right_w = weights_ref[:latent], weights_ref[latent:]
    normed, _ = standardized(align_ref[...].reshape(share * amino, width))
    normed = normed.astype(BF)
    right = lax.dot_general(normed, right_w, NT, preferred_element_type=F32)
    right_ref[...] = right.astype(BF).reshape(right_ref.shape)
    for s in range(share):
        rows = normed[s * amino : (s + 1) * amino]
        left_ref[s] = lax.dot_general(left_w, rows, NT, preferred_element_type=F32).astype(BF)


def panels_of(align, weights):
    share, amino, width = align.shape
    latent = weights.shape[0] // 2
    whole = pl.BlockSpec((2 * latent, width), lambda g: (0, 0))
    return pl.pallas_call(
        panels_kernel,
        grid=(share // 8,),
        in_specs=[pl.BlockSpec((8, amino, width), lambda g: (g, 0, 0)), whole],
        out_specs=[
            pl.BlockSpec((8, latent, amino), lambda g: (g, 0, 0)),
            pl.BlockSpec((8, amino, latent), lambda g: (g, 0, 0)),
        ],
        out_shape=[
            jax.ShapeDtypeStruct((share, latent, amino), BF),
            jax.ShapeDtypeStruct((share, amino, latent), BF),
        ],
        compiler_params=pltpu.CompilerParams(vmem_limit_bytes=24 << 20),
        name="panels",
    )(align, weights)


def align_kernel(align_ref, left_ref, right_ref, weights_ref, out_ref):
    share, amino, width = align_ref.shape
    latent = weights_ref.shape[0] // 2
    left_w, right_w = weights_ref[:latent], weights_ref[latent:]
    normed, factor = standardized(align_ref[...].reshape(share * amino, width))
    grad = jnp.concatenate([lax.dot_general(left_ref[s], left_w, TN, preferred_element_type=F32) for s in range(share)])
    right = right_ref[...].reshape(share * amino, latent)
    grad = grad + jnp.dot(right, right_w, preferred_element_type=F32)
    result = factor * (grad - lane_mean(grad) - normed * lane_mean(grad * normed))
    out_ref[...] = result.reshape(out_ref.shape)


def align_of(align, left_grad, right_grad, weights):
    share, amino, width = align.shape
    latent = weights.shape[0] // 2
    whole = pl.BlockSpec((2 * latent, width), lambda g: (0, 0))
    return pl.pallas_call(
        align_kernel,
        grid=(share // 8,),
        in_specs=[
            pl.BlockSpec((8, amino, width), lambda g: (g, 0, 0)),
            pl.BlockSpec((8, latent, amino), lambda g: (g, 0, 0)),
            pl.BlockSpec((8, amino, latent), lambda g: (g, 0, 0)),
            whole,
        ],
        out_specs=pl.BlockSpec((8, amino, width), lambda g: (g, 0, 0)),
        out_shape=jax.ShapeDtypeStruct(align.shape, F32),
        compiler_params=pltpu.CompilerParams(vmem_limit_bytes=24 << 20),
        name="align",
    )(align, left_grad, right_grad, weights)


def swap_blocks(tiles):
    t0, t1, t2, t3 = tiles
    lane = lax.broadcasted_iota(jnp.int32, t0.shape, 1)
    half, quarter = (lane & 64) == 0, (lane & 32) == 0
    a0, a2 = jnp.where(half, t0, pltpu.roll(t2, 64, 1)), jnp.where(half, pltpu.roll(t0, 64, 1), t2)
    a1, a3 = jnp.where(half, t1, pltpu.roll(t3, 64, 1)), jnp.where(half, pltpu.roll(t1, 64, 1), t3)
    return (
        jnp.where(quarter, a0, pltpu.roll(a1, 32, 1)),
        jnp.where(quarter, pltpu.roll(a0, 96, 1), a1),
        jnp.where(quarter, a2, pltpu.roll(a3, 32, 1)),
        jnp.where(quarter, pltpu.roll(a2, 96, 1), a3),
    )


def grad_outer_kernel(scale, adj_ref, final_ref, right_ref, outer_ref, left_ref):
    quarter, block_i, width = adj_ref.shape
    final = final_ref[...]
    outer_ref = outer_ref.at[pl.ds(pl.program_id(0) * 8 * block_i, 8 * block_i)]
    for four in range(quarter // 4):
        adj = adj_ref[four * 4 : (four + 1) * 4].reshape(4 * block_i, width)
        g = lax.dot_general(adj, final, NT, preferred_element_type=F32).astype(BF)
        for part in range(final.shape[0] // 128):
            tiles = [g[j * block_i : (j + 1) * block_i, part * 128 : (part + 1) * 128] for j in range(4)]
            for c, tile in enumerate(swap_blocks(tiles)):
                at = (part * 4 + c) * block_i
                outer_ref[at : at + block_i, four * 128 : (four + 1) * 128] = tile
    left = lax.dot_general(right_ref[...], outer_ref[...], NT, preferred_element_type=F32)
    left_ref[...] = (left * scale).astype(BF)


def grad_outer_of(adj, final, right, scale):
    _, block_i, width = adj.shape
    seqs, lanes = right.shape
    groups = final.shape[0] // 256
    return pl.pallas_call(
        lambda *refs: grad_outer_kernel(scale, *refs),
        grid=(groups,),
        in_specs=[
            pl.BlockSpec(adj.shape, lambda g: (0, 0, 0)),
            pl.BlockSpec((256, width), lambda g: (g, 0)),
            pl.BlockSpec(right.shape, lambda g: (0, 0)),
        ],
        out_specs=[
            pl.BlockSpec(memory_space=pltpu.VMEM),
            pl.BlockSpec((seqs, 8 * block_i), lambda g: (0, g)),
        ],
        out_shape=[
            pltpu.VMEM((groups * 8 * block_i, lanes), BF),
            jax.ShapeDtypeStruct((seqs, groups * 8 * block_i), BF),
        ],
        compiler_params=pltpu.CompilerParams(vmem_limit_bytes=24 << 20),
        name="grad_outer",
    )(adj, final, right)


def outer_kernel(scale, left_ref, right_ref, adj_ref, final_ref, offset_ref, pair_ref, weight_ref, outer_ref):
    step = pl.program_id(0)
    quarter, block_i, width = adj_ref.shape
    column = pl.ds(pl.multiple_of(step * 128, 128), 128)
    left = left_ref[...]
    for pair in range(quarter // 8):
        o = lax.dot_general(left, right_ref[:, pair * 256 : (pair + 1) * 256], TN, preferred_element_type=F32).astype(BF)
        for part in range(2):
            tiles = [o[c * block_i : (c + 1) * block_i, part * 128 : (part + 1) * 128] for c in range(4)]
            for j, tile in enumerate(swap_blocks(tiles)):
                at = ((pair * 2 + part) * 4 + j) * block_i
                outer_ref[at : at + block_i, column] = tile

    @pl.when(step == pl.num_programs(0) - 1)
    def _():
        weight = None
        for pair in range(quarter // 8):
            rows = slice(pair * 8 * block_i, (pair + 1) * 8 * block_i)
            outer = outer_ref[rows, :]
            adj = adj_ref[pair * 8 : (pair + 1) * 8].reshape(8 * block_i, width)
            pairs = jnp.dot(outer, final_ref[...], preferred_element_type=F32) * scale + offset_ref[...]
            pair_ref[pair * 8 : (pair + 1) * 8] = pairs.astype(BF).reshape(8, block_i, width)
            part = lax.dot_general(adj, outer, TN, preferred_element_type=F32)
            weight = part if weight is None else weight + part
        weight = (weight * scale).T.astype(BF)
        bias = jnp.sum(adj_ref[...].astype(F32).reshape(quarter * block_i, width), axis=0, keepdims=True)
        bias = jnp.broadcast_to(bias.astype(BF), (8, width))
        pieces, rows = weight_ref.shape[0], weight_ref.shape[1] - 8
        for p in range(pieces):
            weight_ref[p] = jnp.concatenate([weight[p * rows : (p + 1) * rows], bias])


def outer_of(left, right, adj, final, offset, scale, pieces):
    quarter, block_i, width = adj.shape
    weight = (pieces, final.shape[0] // pieces + 8, width)
    seqs = left.shape[0]
    whole = lambda shape: pl.BlockSpec(shape, lambda g: (0,) * len(shape))
    return pl.pallas_call(
        lambda *refs: outer_kernel(scale, *refs),
        grid=(left.shape[1] // (4 * block_i),),
        in_specs=[
            pl.BlockSpec((seqs, 4 * block_i), lambda g: (0, g)),
            whole(right.shape),
            whole(adj.shape),
            whole(final.shape),
            whole((1, width)),
        ],
        out_specs=[whole(adj.shape), whole(weight)],
        out_shape=[jax.ShapeDtypeStruct(adj.shape, BF), jax.ShapeDtypeStruct(weight, BF)],
        scratch_shapes=[pltpu.VMEM((quarter * block_i, final.shape[0]), BF)],
        compiler_params=pltpu.CompilerParams(vmem_limit_bytes=24 << 20),
        name="outer",
    )(left, right, adj, final, offset.reshape(1, width))


def shifted(value, axis, by):
    n = lax.axis_size(axis)
    return lax.ppermute(value, axis, [(q, (q + by) % n) for q in range(n)])


def crossings():
    pairs = []
    for row in range(8):
        for col in range(8):
            source_row = ((row + 2 - col // 2 - row % 2) % 4) * 2 + col % 2
            pairs.append((source_row * 8 + row, row * 8 + col))
    return pairs


def exchange(pieces, axis):
    return lax.all_to_all(pieces, axis, split_axis=0, concat_axis=0, tiled=True)


def copies(piece, n):
    return jnp.broadcast_to(piece[None], (n, *piece.shape))


def step(alignment_matrix, twin_linear_matrix, final_matrix, final_offset, adjoint_incoming):
    share, amino, _ = alignment_matrix.shape
    latent = twin_linear_matrix.shape[1] // 2
    depth_count = lax.axis_size("depth")
    row_count = lax.axis_size("row")
    plane_count = row_count * lax.axis_size("col")
    crop_length = amino * lax.axis_size("col")
    _, quarter, width = adjoint_incoming.shape
    kron = final_matrix.shape[0]
    seq_count = share * depth_count
    depth_idx = lax.axis_index("depth")
    there = crossings()
    back = [(b, a) for a, b in there]

    weights_t = twin_linear_matrix.T
    left_own, right_own = panels_of(alignment_matrix, weights_t)
    left_mine = lax.ppermute(left_own.reshape(share, latent * amino), PLANE, there)
    right_own = right_own.reshape(share, depth_count, quarter * latent).transpose(1, 0, 2)
    right = exchange(right_own, "depth")

    def turned_back(chunks):
        chunks = chunks.reshape(depth_count, share, -1)[::-1]
        start = depth_count - 1 - depth_idx
        return lax.dynamic_slice_in_dim(jnp.concatenate([chunks, chunks]), start, depth_count, 0)

    right_turned = turned_back(right).reshape(seq_count, quarter * latent)
    right = right.reshape(seq_count, quarter * latent)

    adj = jnp.transpose(adjoint_incoming, (1, 0, 2))
    adj, left_mine = lax.optimization_barrier((adj, left_mine))
    left = jnp.concatenate([left_mine] + [shifted(left_mine, "depth", k) for k in range(1, depth_count)])
    grad_outer, grad_left = grad_outer_of(adj, final_matrix, right, 1.0 / seq_count)
    grad_right = lax.dot_general(left, grad_outer, (((1,), (0,)), ((), ())), preferred_element_type=F32)
    grad_right = (grad_right / seq_count).astype(BF)
    grad_left = grad_left.reshape(depth_count, share, latent * amino)
    grads = exchange(jnp.concatenate([grad_left, turned_back(grad_right)], axis=-1), "depth")
    pair_t, weight = outer_of(left, right_turned, adj, final_matrix, final_offset, 1.0 / seq_count, plane_count)
    contact_delta = jnp.transpose(pair_t, (1, 0, 2))

    left_sum = jnp.sum(grads[..., : latent * amino].astype(F32), axis=0).astype(BF)
    weight, left_sum = lax.optimization_barrier((weight, left_sum))
    left_part = lax.ppermute(left_sum, PLANE, back)
    piece = latent * amino // row_count
    left_pieces = left_part.reshape(share, row_count, piece).transpose(1, 0, 2)
    right_pieces = grads[..., latent * amino :].reshape(depth_count, share, row_count // depth_count, piece)
    right_pieces = right_pieces.transpose(0, 2, 1, 3).reshape(row_count, share, piece)
    pieces = jnp.concatenate([left_pieces, right_pieces], axis=-1)
    turned = lax.dynamic_slice_in_dim(jnp.concatenate([pieces, pieces]), lax.axis_index("row"), row_count, 0)
    reduced = turned[0].astype(F32)
    for k in range(1, row_count):
        reduced = reduced + shifted(turned[k], "row", k).astype(F32)
    reduced = reduced.astype(BF)
    grads = exchange(copies(reduced, row_count), "row")
    left_full = grads[..., :piece].reshape(row_count, share, latent // row_count, amino)
    left_full = left_full.transpose(1, 0, 2, 3).reshape(share, latent, amino)
    right_full = grads[..., piece:].reshape(row_count, share, amino // row_count, latent)
    right_full = right_full.transpose(1, 0, 2, 3).reshape(share, amino, latent)
    alignment_adjoint = align_of(alignment_matrix, left_full, right_full, weights_t)

    rows = kron // plane_count
    received = exchange(weight, PLANE)
    mine = jnp.sum(received.astype(F32), axis=0)
    total = ((mine + shifted(mine, "depth", 2)) + (shifted(mine, "depth", 1) + shifted(mine, "depth", 3))) / crop_length
    total, contact_delta = lax.optimization_barrier((total, contact_delta))
    weight_gradient = exchange(copies(total[:rows].astype(BF), plane_count), PLANE)
    weight_gradient = weight_gradient.reshape(kron, width).astype(F32)
    return contact_delta, alignment_adjoint, weight_gradient, total[rows]


def solution(mesh):
    in_specs = (P("depth", "col", None), P(), P(), P(), P("row", ("col", "depth"), None))
    out_specs = (P("row", ("col", "depth"), None), P("depth", "col", None), P(), P())
    return jax.shard_map(step, mesh=mesh, in_specs=in_specs, out_specs=out_specs, check_vma=False)
```

```python
import jax
import jax.numpy as jnp
from jax import lax
from jax.experimental import pallas as pl
from jax.experimental.pallas import tpu as pltpu
from jax.sharding import PartitionSpec as P


epsilon = 1e-05
BF, F32 = jnp.bfloat16, jnp.float32
PLANE = ("row", "col")
TN = (((0,), (0,)), ((), ()))
NT = (((1,), (1,)), ((), ()))


def lane_mean(values):
    return jnp.mean(values.astype(F32), axis=-1, keepdims=True)


def standardized(rows):
    centred = rows.astype(F32) - lane_mean(rows)
    factor = lax.rsqrt(lane_mean(jnp.square(centred)) + epsilon)
    return centred * factor, factor


def panels_kernel(align_ref, weights_ref, left_ref, right_ref):
    share, amino, width = align_ref.shape
    latent = weights_ref.shape[0] // 2
    left_w, right_w = weights_ref[:latent], weights_ref[latent:]
    normed, _ = standardized(align_ref[...].reshape(share * amino, width))
    normed = normed.astype(BF)
    right = lax.dot_general(normed, right_w, NT, preferred_element_type=F32)
    right_ref[...] = right.astype(BF).reshape(right_ref.shape)
    for s in range(share):
        rows = normed[s * amino : (s + 1) * amino]
        left_ref[s] = lax.dot_general(left_w, rows, NT, preferred_element_type=F32).astype(BF)


def panels_of(align, weights):
    share, amino, width = align.shape
    latent = weights.shape[0] // 2
    whole = pl.BlockSpec((2 * latent, width), lambda g: (0, 0))
    return pl.pallas_call(
        panels_kernel,
        grid=(share // 8,),
        in_specs=[pl.BlockSpec((8, amino, width), lambda g: (g, 0, 0)), whole],
        out_specs=[
            pl.BlockSpec((8, latent, amino), lambda g: (g, 0, 0)),
            pl.BlockSpec((8, amino, latent), lambda g: (g, 0, 0)),
        ],
        out_shape=[
            jax.ShapeDtypeStruct((share, latent, amino), BF),
            jax.ShapeDtypeStruct((share, amino, latent), BF),
        ],
        compiler_params=pltpu.CompilerParams(vmem_limit_bytes=24 << 20),
        name="panels",
    )(align, weights)


def align_kernel(align_ref, left_ref, right_ref, weights_ref, out_ref):
    share, amino, width = align_ref.shape
    latent = weights_ref.shape[0] // 2
    left_w, right_w = weights_ref[:latent], weights_ref[latent:]
    normed, factor = standardized(align_ref[...].reshape(share * amino, width))
    grad = jnp.concatenate([lax.dot_general(left_ref[s], left_w, TN, preferred_element_type=F32) for s in range(share)])
    right = right_ref[...].reshape(share * amino, latent)
    grad = grad + jnp.dot(right, right_w, preferred_element_type=F32)
    result = factor * (grad - lane_mean(grad) - normed * lane_mean(grad * normed))
    out_ref[...] = result.reshape(out_ref.shape)


def align_of(align, left_grad, right_grad, weights):
    share, amino, width = align.shape
    latent = weights.shape[0] // 2
    whole = pl.BlockSpec((2 * latent, width), lambda g: (0, 0))
    return pl.pallas_call(
        align_kernel,
        grid=(share // 8,),
        in_specs=[
            pl.BlockSpec((8, amino, width), lambda g: (g, 0, 0)),
            pl.BlockSpec((8, latent, amino), lambda g: (g, 0, 0)),
            pl.BlockSpec((8, amino, latent), lambda g: (g, 0, 0)),
            whole,
        ],
        out_specs=pl.BlockSpec((8, amino, width), lambda g: (g, 0, 0)),
        out_shape=jax.ShapeDtypeStruct(align.shape, F32),
        compiler_params=pltpu.CompilerParams(vmem_limit_bytes=24 << 20),
        name="align",
    )(align, left_grad, right_grad, weights)


def swap_blocks(tiles):
    t0, t1, t2, t3 = tiles
    lane = lax.broadcasted_iota(jnp.int32, t0.shape, 1)
    half, quarter = (lane & 64) == 0, (lane & 32) == 0
    a0, a2 = jnp.where(half, t0, pltpu.roll(t2, 64, 1)), jnp.where(half, pltpu.roll(t0, 64, 1), t2)
    a1, a3 = jnp.where(half, t1, pltpu.roll(t3, 64, 1)), jnp.where(half, pltpu.roll(t1, 64, 1), t3)
    return (
        jnp.where(quarter, a0, pltpu.roll(a1, 32, 1)),
        jnp.where(quarter, pltpu.roll(a0, 96, 1), a1),
        jnp.where(quarter, a2, pltpu.roll(a3, 32, 1)),
        jnp.where(quarter, pltpu.roll(a2, 96, 1), a3),
    )


def grad_outer_kernel(scale, adj_ref, final_ref, right_ref, outer_ref, left_ref):
    quarter, block_i, width = adj_ref.shape
    final = final_ref[...]
    outer_ref = outer_ref.at[pl.ds(pl.program_id(0) * 8 * block_i, 8 * block_i)]
    for four in range(quarter // 4):
        adj = adj_ref[four * 4 : (four + 1) * 4].reshape(4 * block_i, width)
        g = lax.dot_general(adj, final, NT, preferred_element_type=F32).astype(BF)
        for part in range(final.shape[0] // 128):
            tiles = [g[j * block_i : (j + 1) * block_i, part * 128 : (part + 1) * 128] for j in range(4)]
            for c, tile in enumerate(swap_blocks(tiles)):
                at = (part * 4 + c) * block_i
                outer_ref[at : at + block_i, four * 128 : (four + 1) * 128] = tile
    left = lax.dot_general(right_ref[...], outer_ref[...], NT, preferred_element_type=F32)
    left_ref[...] = (left * scale).astype(BF)


def grad_outer_of(adj, final, right, scale):
    _, block_i, width = adj.shape
    seqs, lanes = right.shape
    groups = final.shape[0] // 256
    return pl.pallas_call(
        lambda *refs: grad_outer_kernel(scale, *refs),
        grid=(groups,),
        in_specs=[
            pl.BlockSpec(adj.shape, lambda g: (0, 0, 0)),
            pl.BlockSpec((256, width), lambda g: (g, 0)),
            pl.BlockSpec(right.shape, lambda g: (0, 0)),
        ],
        out_specs=[
            pl.BlockSpec(memory_space=pltpu.VMEM),
            pl.BlockSpec((seqs, 8 * block_i), lambda g: (0, g)),
        ],
        out_shape=[
            pltpu.VMEM((groups * 8 * block_i, lanes), BF),
            jax.ShapeDtypeStruct((seqs, groups * 8 * block_i), BF),
        ],
        compiler_params=pltpu.CompilerParams(vmem_limit_bytes=24 << 20),
        name="grad_outer",
    )(adj, final, right)


def outer_kernel(scale, left_ref, right_ref, adj_ref, final_ref, offset_ref, pair_ref, weight_ref, outer_ref):
    step = pl.program_id(0)
    quarter, block_i, width = adj_ref.shape
    column = pl.ds(pl.multiple_of(step * 128, 128), 128)
    left = left_ref[...]
    for pair in range(quarter // 8):
        o = lax.dot_general(left, right_ref[:, pair * 256 : (pair + 1) * 256], TN, preferred_element_type=F32).astype(BF)
        for part in range(2):
            tiles = [o[c * block_i : (c + 1) * block_i, part * 128 : (part + 1) * 128] for c in range(4)]
            for j, tile in enumerate(swap_blocks(tiles)):
                at = ((pair * 2 + part) * 4 + j) * block_i
                outer_ref[at : at + block_i, column] = tile

    @pl.when(step == pl.num_programs(0) - 1)
    def _():
        weight = None
        for pair in range(quarter // 8):
            rows = slice(pair * 8 * block_i, (pair + 1) * 8 * block_i)
            outer = outer_ref[rows, :]
            adj = adj_ref[pair * 8 : (pair + 1) * 8].reshape(8 * block_i, width)
            pairs = jnp.dot(outer, final_ref[...], preferred_element_type=F32) * scale + offset_ref[...]
            pair_ref[pair * 8 : (pair + 1) * 8] = pairs.astype(BF).reshape(8, block_i, width)
            part = lax.dot_general(adj, outer, TN, preferred_element_type=F32)
            weight = part if weight is None else weight + part
        weight = (weight * scale).T.astype(BF)
        bias = jnp.sum(adj_ref[...].astype(F32).reshape(quarter * block_i, width), axis=0, keepdims=True)
        bias = jnp.broadcast_to(bias.astype(BF), (8, width))
        pieces, rows = weight_ref.shape[0], weight_ref.shape[1] - 8
        for p in range(pieces):
            weight_ref[p] = jnp.concatenate([weight[p * rows : (p + 1) * rows], bias])


def outer_of(left, right, adj, final, offset, scale, pieces):
    quarter, block_i, width = adj.shape
    weight = (pieces, final.shape[0] // pieces + 8, width)
    seqs = left.shape[0]
    whole = lambda shape: pl.BlockSpec(shape, lambda g: (0,) * len(shape))
    return pl.pallas_call(
        lambda *refs: outer_kernel(scale, *refs),
        grid=(left.shape[1] // (4 * block_i),),
        in_specs=[
            pl.BlockSpec((seqs, 4 * block_i), lambda g: (0, g)),
            whole(right.shape),
            whole(adj.shape),
            whole(final.shape),
            whole((1, width)),
        ],
        out_specs=[whole(adj.shape), whole(weight)],
        out_shape=[jax.ShapeDtypeStruct(adj.shape, BF), jax.ShapeDtypeStruct(weight, BF)],
        scratch_shapes=[pltpu.VMEM((quarter * block_i, final.shape[0]), BF)],
        compiler_params=pltpu.CompilerParams(vmem_limit_bytes=24 << 20),
        name="outer",
    )(left, right, adj, final, offset.reshape(1, width))


def shifted(value, axis, by):
    n = lax.axis_size(axis)
    return lax.ppermute(value, axis, [(q, (q + by) % n) for q in range(n)])


def crossings():
    pairs = []
    for row in range(8):
        for col in range(8):
            source_row = ((row + 2 - col // 2 - row % 2) % 4) * 2 + col % 2
            pairs.append((source_row * 8 + row, row * 8 + col))
    return pairs


def exchange(pieces, axis):
    return lax.all_to_all(pieces, axis, split_axis=0, concat_axis=0, tiled=True)


def copies(piece, n):
    return jnp.broadcast_to(piece[None], (n, *piece.shape))


def step(alignment_matrix, twin_linear_matrix, final_matrix, final_offset, adjoint_incoming):
    share, amino, _ = alignment_matrix.shape
    latent = twin_linear_matrix.shape[1] // 2
    depth_count = lax.axis_size("depth")
    row_count = lax.axis_size("row")
    plane_count = row_count * lax.axis_size("col")
    crop_length = amino * lax.axis_size("col")
    _, quarter, width = adjoint_incoming.shape
    kron = final_matrix.shape[0]
    seq_count = share * depth_count
    depth_idx = lax.axis_index("depth")
    there = crossings()
    back = [(b, a) for a, b in there]

    weights_t = twin_linear_matrix.T
    left_own, right_own = panels_of(alignment_matrix, weights_t)
    left_mine = lax.ppermute(left_own.reshape(share, latent * amino), PLANE, there)
    right_own = right_own.reshape(share, depth_count, quarter * latent).transpose(1, 0, 2)
    right = exchange(right_own, "depth")

    def turned_back(chunks):
        chunks = chunks.reshape(depth_count, share, -1)[::-1]
        start = depth_count - 1 - depth_idx
        return lax.dynamic_slice_in_dim(jnp.concatenate([chunks, chunks]), start, depth_count, 0)

    right = turned_back(right).reshape(seq_count, quarter * latent)

    adj = jnp.transpose(adjoint_incoming, (1, 0, 2))
    adj, left_mine = lax.optimization_barrier((adj, left_mine))
    left = jnp.concatenate([left_mine] + [shifted(left_mine, "depth", k) for k in range(1, depth_count)])
    grad_outer, grad_left = grad_outer_of(adj, final_matrix, right, 1.0 / seq_count)
    grad_right = lax.dot_general(left, grad_outer, (((1,), (0,)), ((), ())), preferred_element_type=F32)
    grad_right = (grad_right / seq_count).astype(BF)
    grads = jnp.concatenate([grad_left, grad_right], axis=-1).reshape(depth_count, share, -1)
    grads = [grads[0]] + [shifted(grads[k], "depth", -k) for k in range(1, depth_count)]
    pair_t, weight = outer_of(left, right, adj, final_matrix, final_offset, 1.0 / seq_count, plane_count)
    contact_delta = jnp.transpose(pair_t, (1, 0, 2))

    left_sum = sum(g[:, : latent * amino].astype(F32) for g in grads).astype(BF)
    weight, left_sum = lax.optimization_barrier((weight, left_sum))
    left_part = lax.ppermute(left_sum, PLANE, back)
    piece = latent * amino // row_count
    left_pieces = left_part.reshape(share, row_count, piece).transpose(1, 0, 2)
    row_idx = lax.axis_index("row")
    right_pieces = jnp.concatenate([g[:, latent * amino :] for g in grads] * 2, axis=-1)
    right_start = (row_idx - depth_idx * (row_count // depth_count)) % row_count
    right_turned = lax.dynamic_slice_in_dim(right_pieces, right_start * piece, row_count * piece, 1)
    left_turned = lax.dynamic_slice_in_dim(jnp.concatenate([left_pieces, left_pieces]), row_idx, row_count, 0)
    turned = [
        jnp.concatenate([left_turned[k], right_turned[:, k * piece : (k + 1) * piece]], axis=-1)
        for k in range(row_count)
    ]
    reduced = turned[0].astype(F32)
    for k in range(1, row_count):
        reduced = reduced + shifted(turned[k], "row", k).astype(F32)
    reduced = reduced.astype(BF)
    grads = exchange(copies(reduced, row_count), "row")
    left_full = grads[..., :piece].reshape(row_count, share, latent // row_count, amino)
    left_full = left_full.transpose(1, 0, 2, 3).reshape(share, latent, amino)
    right_full = grads[..., piece:].reshape(row_count, share, amino // row_count, latent)
    right_full = right_full.transpose(1, 0, 2, 3).reshape(share, amino, latent)
    alignment_adjoint = align_of(alignment_matrix, left_full, right_full, weights_t)

    rows = kron // plane_count
    received = exchange(weight, PLANE)
    mine = jnp.sum(received.astype(F32), axis=0)
    total = ((mine + shifted(mine, "depth", 2)) + (shifted(mine, "depth", 1) + shifted(mine, "depth", 3))) / crop_length
    total, contact_delta = lax.optimization_barrier((total, contact_delta))
    weight_gradient = exchange(copies(total[:rows].astype(BF), plane_count), PLANE)
    weight_gradient = weight_gradient.reshape(kron, width).astype(F32)
    return contact_delta, alignment_adjoint, weight_gradient, total[rows]


def solution(mesh):
    in_specs = (P("depth", "col", None), P(), P(), P(), P("row", ("col", "depth"), None))
    out_specs = (P("row", ("col", "depth"), None), P("depth", "col", None), P(), P())
    return jax.shard_map(step, mesh=mesh, in_specs=in_specs, out_specs=out_specs, check_vma=False)
```
